256 devices in a mesh: row: 16 (over x, z_hi), col: 8 (over y, core), ga: 2 (over z_lo).
Axes of the slice: x: 4, y: 4, z: 8 (z_hi: 4, z_lo: 2; z = z_hi * 2 + z_lo), core: 2. Of those that a mesh axis runs over, the one named last changes fastest.
Arguments:
- pair_density: float32 [512, 24, 3072], P('row', None, 'ga'), may hold values from -6 to 6
- coulomb: float32 [3072], P('ga'), may hold values from 0.1 to 2
Outputs:
- kernel: float32 [12288, 12288], P('row', 'col')
The draws below stay inside these ranges and needn't reach their ends.
All inputs are finite; a program needn't handle non-finite values.
Results may differ from the reference program's by a relative error of at most 0.00011.
Values sent between devices are 32-bit elements; how exact they have to be, the bound alone decides.
A program may use at most 64 MiB of HBM per device.

```python
import math
import jax
import jax.numpy as jnp
from jax import lax

NG = 3072
NK = 512
NVC = 24
N_ROW = 16
N_COL = 8


def level_of(own_key, extent, cuts, low, top_value):
    gain, own = 1.0, jax.random.fold_in(own_key, 6)
    for position, blocks in cuts:
        steps = jnp.exp(jax.random.uniform(jax.random.fold_in(own, position), (blocks,), jnp.float32, low / len(cuts), top_value / len(cuts)))
        gain = gain * jnp.repeat(steps, extent[position] // blocks).reshape([-1 if axis == position else 1 for axis in range(len(extent))])
    return gain


def bell_draw(rng, shape, spread, limit, split=(), kind=jnp.bfloat16):
    drawn = spread * jax.random.normal(rng, shape, jnp.float32)
    if split:
        drawn = drawn * level_of(rng, shape, split, -0.22, 0.18)
    return jnp.clip(drawn, -limit, limit).astype(kind)


def setup_inputs(seed: int = 0) -> dict:
    key_of = jax.random.split(jax.random.key(seed), 3)
    pair_density = bell_draw(key_of[0], (NK, NVC, NG), 1.0, 6.0, ((0, 16), (2, 2)), jnp.float32)
    coulomb = jnp.clip(jnp.exp(math.log(2.0) - 2.9957323 * jax.random.uniform(key_of[1], (NG,), jnp.float32) ** level_of(key_of[1], (NG,), ((0, 2),), -0.2, 0.2)), 0.1, 2.0)
    return {"pair_density": pair_density, "coulomb": coulomb}


def contract(left_rows, right_rows):
    return lax.dot_general(left_rows, right_rows, (((1,), (1,)), ((), ())), precision=lax.Precision.HIGHEST, preferred_element_type=jnp.float32)


def reference(pair_density, coulomb):
    row_order = jnp.arange(NK, dtype=jnp.int32).reshape(NK // N_ROW, N_ROW).T.reshape(-1)
    col_order = jnp.arange(NK, dtype=jnp.int32).reshape(NK // N_COL, N_COL).T.reshape(-1)
    left = pair_density[row_order]
    right = pair_density[col_order]
    bands = pair_density.shape[1]
    g_width = pair_density.shape[2]
    weighted = left.reshape(NK * bands, g_width) * (2.0 * coulomb)[None, :]
    exchange = contract(weighted, right.reshape(NK * bands, g_width))
    return exchange / jnp.float32(NK)
```

```python
import jax
import jax.numpy as jnp
from jax import lax
from jax.experimental import pallas as pl
from jax.experimental.pallas import tpu as pltpu
from jax.sharding import PartitionSpec as P

MESH = pl.DeviceIdType.MESH
F32 = jnp.float32
BF16 = jnp.bfloat16

LAG = 2
PLAN = (
    (0, 0, -1, -1),
    (2, 2, -1, -1),
    (3, 3, 2, 1),
    (1, 1, 1, 3),
    (30, 30, 3, 5),
    (96, 7, 0, 0),
    (7, 31, 31, 7),
    (4, 4, 30, 4),
    (28, 28, 28, 9),
    (31, 29, 29, 2),
    (8, 8, 26, 11),
    (6, 6, 24, 6),
    (24, 24, 27, 8),
    (98, 5, 25, 10),
    (29, 10, 23, 12),
    (5, 26, 21, 14),
    (26, 35, 61, 37),
    (10, 11, 63, 101),
    (100, 60, 57, 41),
    (97, 12, 59, 43),
    (27, 20, 53, 105),
    (11, 62, 55, 42),
    (25, 38, 123, 109),
    (20, 22, 122, 107),
    (12, 39, 121, 46),
    (14, 63, 52, 111),
    (104, 56, 118, 65),
    (16, 58, 65, 71),
    (106, 59, 88, 69),
    (108, 57, 90, 75),
    (110, 48, 91, 73),
    (113, 50, 89, 79),
)
STEPS = ((1, 0), (-1, 0), (0, 1), (0, -1))
NX, NZ, NY = 4, 8, 4
GROUP_ORDER = (0, 1, 3, 2)
M_TILE = 256

AT_ROWS, AT_PAIR, AT_FIRST, AT_SECOND, AT_RELAY, AT_CORE = 5, 8, 10, 14, 18, 20
UNITS = {21: 1, 22: 1, 23: 1, 24: 1, 25: 1, 26: 1, 27: 3, 28: 3, 29: 2, 30: 2, 31: 2}


def split(value):
    high = value.astype(BF16)
    return high, (value - high.astype(F32)).astype(BF16)


def contract(left, right):
    return lax.dot_general(
        left, right, (((1,), (1,)), ((), ())), preferred_element_type=F32
    )


def kernel(
    pairs, scale, out,
    cols, rows, scales, left_hi, left_lo, right_hi, right_lo, total,
    col_send, col_recv, row_send, row_recv, sub_send, sub_recv, own_sem, out_sem,
):
    row, col, half = lax.axis_index("row"), lax.axis_index("col"), lax.axis_index("ga")
    x, y, core = row // 4, col // 2, col % 2
    z = 2 * (row % 4) + half
    other = 1 - half
    width = pairs.shape[2]
    quarter = width // NY
    bands = pairs.shape[1]
    n_row = 16

    def place(xx, zz, cc=None):
        return {"row": 4 * xx + zz // 2, "col": col if cc is None else cc, "ga": zz % 2}

    def near(step):
        return place((x + step[0] + NX) % NX, (z + step[1] + NZ) % NZ)

    y_up = {"row": row, "col": (col + 2) % 8, "ga": half}
    y_down = {"row": row, "col": (col + 6) % 8, "ga": half}
    twin = {"row": row, "col": 2 * y + 1 - core, "ga": half}
    pair = {"row": row, "col": col, "ga": other}
    z_out = near((0, 1)), near((0, -1))

    def remote(src, dst, send, recv, device):
        return pltpu.make_async_remote_copy(
            src_ref=src, dst_ref=dst, send_sem=send, recv_sem=recv,
            device_id=device, device_id_type=MESH,
        )

    barrier = pltpu.get_barrier_semaphore()
    for step in range(1, n_row):
        pl.semaphore_signal(
            barrier, inc=1, device_id={"row": (row + step) % n_row, "col": col, "ga": half},
            device_id_type=MESH,
        )
    for device in (*z_out, y_up, y_down, twin):
        pl.semaphore_signal(barrier, inc=1, device_id=device, device_id_type=MESH)

    lanes = pl.ds(pl.multiple_of(y * quarter, 128), quarter)
    own_rows = pltpu.make_async_copy(
        pairs.at[row + 16 * core, :, lanes], rows.at[half, y, core, row], own_sem.at[0]
    )
    own_rows.start()
    own_scale = pltpu.make_async_copy(scale, scales.at[half], own_sem.at[1])
    own_scale.start()
    own_cols = []
    for piece in range(4):
        own_cols.append(pltpu.make_async_copy(
            pairs.at[col + 8 * piece], cols.at[half, 4 * row + piece], own_sem.at[2 + piece]
        ))
        own_cols[-1].start()

    pl.semaphore_wait(barrier, n_row - 1 + 5)

    sends = []

    def go(copy):
        copy.start()
        sends.append(copy)

    go(remote(scale, scales.at[half], sub_send.at[0], sub_recv.at[0], pair))
    for step in range(1, n_row):
        to = (row + step) % n_row
        go(remote(
            pairs.at[to + 16 * core, :, lanes], rows.at[half, y, core, row],
            row_send.at[step], row_recv.at[step], {"row": to, "col": col, "ga": half},
        ))

    def slot(code, step=(0, 0)):
        xs = (x + code // 32 - step[0] + NX) % NX
        zs = (z + (code // 4) % 8 - step[1] + NZ) % NZ
        return zs % 2, 4 * (4 * xs + zs // 2) + code % 4

    def send_round(number):
        for way, code in enumerate(PLAN[number]):
            if code < 0:
                continue
            where = cols.at[slot(code)]
            src = pairs.at[col + 8 * (code % 4)] if code < 4 else where
            index = 4 * number + way
            go(remote(src, where, col_send.at[index], col_recv.at[index], near(STEPS[way])))

    def wait_round(number):
        for way, code in enumerate(PLAN[number]):
            if code < 0:
                continue
            where = cols.at[slot(code, STEPS[way])]
            index = 4 * number + way
            remote(
                where, where, col_send.at[index], col_recv.at[index], near(STEPS[way])
            ).wait_recv()

    def part(h, yy, cc):
        return rows.at[h, (yy + NY) % NY, cc]

    def send_part(h, yy, number, device):
        ref = part(h, yy, core)
        go(remote(ref, ref, sub_send.at[number], sub_recv.at[number], device))

    def wait_part(h, yy, cc, number):
        ref = part(h, yy, cc)
        remote(ref, ref, sub_send.at[number], sub_recv.at[number], twin).wait_recv()

    def to_twin(h, yy, number):
        send_part(h, yy, number, twin)

    def exchange(number):
        if number == AT_ROWS:
            own_rows.wait()
            for step in range(1, n_row):
                where = rows.at[half, y, core, (row + n_row - step) % n_row]
                remote(
                    where, where, row_send.at[step], row_recv.at[step], pair
                ).wait_recv()
            send_part(half, y, 1, pair)
            send_part(half, y, 2, y_up)
            send_part(half, y, 3, y_down)
            to_twin(half, y, 8)
        if number == AT_PAIR:
            wait_part(other, y, core, 1)
            send_part(other, y, 4, y_up)
            send_part(other, y, 5, y_down)
            to_twin(other, y, 9)
        if number == AT_FIRST:
            wait_part(half, y - 1, core, 2)
            send_part(half, y - 1, 6, y_up)
            to_twin(half, y - 1, 10)
            wait_part(half, y + 1, core, 3)
            to_twin(half, y + 1, 11)
        if number == AT_SECOND:
            wait_part(other, y + 1, core, 5)
            send_part(other, y + 1, 7, y_down)
            to_twin(other, y + 1, 12)
            wait_part(other, y - 1, core, 4)
            to_twin(other, y - 1, 13)
        if number == AT_RELAY:
            wait_part(half, y - 2, core, 6)
            to_twin(half, y - 2, 14)
            wait_part(other, y + 2, core, 7)
            to_twin(other, y + 2, 15)
        if number == AT_CORE:
            own_scale.wait()
            remote(scale, scales.at[other], sub_send.at[0], sub_recv.at[0], pair).wait_recv()
            for n, (h, yy) in enumerate((
                (half, y), (other, y), (half, y - 1), (half, y + 1),
                (other, y + 1), (other, y - 1), (half, y - 2), (other, y + 2),
            )):
                wait_part(h, yy, 1 - core, 8 + n)

            def fill(i, carry):
                h, yy, r = i // (NY * n_row), (i // n_row) % NY, i % n_row
                at = pl.ds(pl.multiple_of(yy * quarter, 128), quarter)
                both = jnp.concatenate([rows[h, yy, 0, r], rows[h, yy, 1, r]], axis=0)
                hi, lo = split(both * scales[h, 0:1, at])
                to = pl.ds(pl.multiple_of(r * 2 * bands, 16), 2 * bands)
                left_hi[h, to, at] = hi
                left_lo[h, to, at] = lo
                return carry

            lax.fori_loop(0, 2 * NY * n_row, fill, 0)

    def unit(u, carry):
        group, part_no, tile = u // 6, (u // 3) % 2, u % 3
        ox = group + (group // 2) * (5 - 2 * group)
        xs = (x + ox) % NX
        h = (half + part_no) % 2

        @pl.when(tile == 0)
        def _():
            def fill(i, c):
                block = cols[h, pl.ds(16 * xs + 2 * i, 2)].reshape(2 * bands, width)
                hi, lo = split(block)
                to = pl.ds(pl.multiple_of(i * 2 * bands, 16), 2 * bands)
                right_hi[to, :] = hi
                right_lo[to, :] = lo
                return c

            lax.fori_loop(0, 8, fill, 0)

        m = pl.ds(pl.multiple_of(tile * M_TILE, M_TILE), M_TILE)
        hi, lo = right_hi[...], right_lo[...]
        result = contract(left_hi[h, m, :], hi)
        result += contract(left_hi[h, m, :], lo)
        result += contract(left_lo[h, m, :], hi)

        @pl.when(part_no == 0)
        def _():
            total[group, m, :] = result

        @pl.when(part_no == 1)
        def _():
            total[group, m, :] += result
            at = pl.ds(pl.multiple_of(xs * 16 * bands, 128), 16 * bands)
            pltpu.make_async_copy(
                total.at[group, m, :], out.at[m, at], out_sem.at[3 * group + tile]
            ).start()

        return carry

    rounds = len(PLAN)
    done = 0
    for number in range(rounds):
        if number >= LAG:
            wait_round(number - LAG)
        send_round(number)
        exchange(number)
        count = UNITS.get(number, 0)
        if count:
            if done == 0:
                for copy in own_cols:
                    copy.wait()
            lax.fori_loop(done, done + count, unit, 0)
            done += count
    for number in range(rounds - LAG, rounds):
        wait_round(number)
    lax.fori_loop(done, 24, unit, 0)

    def flush(u, carry):
        group, tile = u // 3, u % 3
        ox = group + (group // 2) * (5 - 2 * group)
        xs = (x + ox) % NX
        m = pl.ds(pl.multiple_of(tile * M_TILE, M_TILE), M_TILE)
        at = pl.ds(pl.multiple_of(xs * 16 * bands, 128), 16 * bands)
        pltpu.make_async_copy(
            total.at[group, m, :], out.at[m, at], out_sem.at[3 * group + tile]
        ).wait()
        return carry

    for copy in sends:
        copy.wait_send()
    lax.fori_loop(0, 12, flush, 0)


def local(pair_density, coulomb):
    local_k, bands, width = pair_density.shape
    n_row = lax.axis_size("row")
    total_k = local_k * n_row
    scale = jnp.broadcast_to((2.0 * coulomb / F32(total_k))[None, :], (8, width))
    m = 2 * n_row * bands
    n = 4 * n_row * bands
    group = n // NX
    rounds = len(PLAN)
    return pl.pallas_call(
        kernel,
        out_shape=jax.ShapeDtypeStruct((m, n), F32),
        in_specs=[pl.BlockSpec(memory_space=pl.ANY), pl.BlockSpec(memory_space=pltpu.VMEM)],
        out_specs=pl.BlockSpec(memory_space=pl.ANY),
        scratch_shapes=[
            pltpu.VMEM((2, 4 * n_row, bands, width), F32),
            pltpu.VMEM((2, NY, 2, n_row, bands, width // NY), F32),
            pltpu.VMEM((2, 8, width), F32),
            pltpu.VMEM((2, m, width), BF16),
            pltpu.VMEM((2, m, width), BF16),
            pltpu.VMEM((group, width), BF16),
            pltpu.VMEM((group, width), BF16),
            pltpu.VMEM((NX, m, group), F32),
            pltpu.SemaphoreType.DMA((4 * rounds,)),
            pltpu.SemaphoreType.DMA((4 * rounds,)),
            pltpu.SemaphoreType.DMA((n_row,)),
            pltpu.SemaphoreType.DMA((n_row,)),
            pltpu.SemaphoreType.DMA((16,)),
            pltpu.SemaphoreType.DMA((16,)),
            pltpu.SemaphoreType.DMA((6,)),
            pltpu.SemaphoreType.DMA((12,)),
        ],
        compiler_params=pltpu.CompilerParams(
            collective_id=0, has_side_effects=True, vmem_limit_bytes=64 * 1024 * 1024 - 2 * 1024 * 1024
        ),
        name="gather_and_contract",
    )(pair_density, scale)


def solution(mesh):
    placed = (P("row", None, "ga"), P("ga"))
    return jax.shard_map(
        local, mesh=mesh, in_specs=placed, out_specs=P("row", "col"), check_vma=False
    )
```

```python
import jax
import jax.numpy as jnp
from jax import lax
from jax.experimental import pallas as pl
from jax.experimental.pallas import tpu as pltpu
from jax.sharding import PartitionSpec as P

MESH = pl.DeviceIdType.MESH
F32 = jnp.float32
BF16 = jnp.bfloat16

LAG = 3
PLAN = (
    (2, 2, -1, -1),
    (1, 1, -1, -1),
    (3, 0, -1, -1),
    (0, 3, 3, 2),
    (97, 34, 0, 3),
    (99, 32, 2, 1),
    (6, 6, 1, 0),
    (28, 7, 28, 6),
    (30, 30, 30, 5),
    (5, 29, 31, 7),
    (10, 10, 29, 4),
    (26, 26, 35, 32),
    (9, 9, 32, 33),
    (25, 25, 26, 99),
    (24, 24, 99, 11),
    (8, 27, 25, 9),
    (22, 22, 27, 10),
    (15, 15, 24, 8),
    (21, 21, 104, 121),
    (14, 14, 21, 39),
    (13, 13, 111, 36),
    (20, 23, 127, 14),
    (17, 17, 20, 15),
    (12, 54, 56, 40),
    (18, 18, 123, 47),
    (16, 16, 67, 67),
    (19, 46, 64, 64),
    (106, 50, 65, 65),
    (122, 49, 66, 66),
    (112, 45, 95, 71),
    (116, 53, 92, 68),
    (108, 51, 93, 69),
    (119, -1, -1, 75),
)
STEPS = ((1, 0), (-1, 0), (0, 1), (0, -1))
NX, NZ, NY = 4, 8, 4
M_TILE = 256
FIRST_LIMIT, LAST_LIMIT = 36 * 2**20, 6 * 2**20

AT_ROWS, AT_PAIR, AT_FIRST, AT_SECOND, AT_RELAY, AT_CORE = 5, 8, 10, 14, 18, 20
PARTS = ((0, 1), (0, 0), (1, 1), (3, 1), (1, 0), (3, 0), (2, 0), (2, 1))
OPENS = (1, 0, 1, 1, 0, 0, 1, 0)
TILES = {21: 1, 22: 1, 23: 1, 25: 2, 26: 2, 27: 2, 28: 2, 29: 2, 30: 2, 31: 2, 32: 1}
EARLY = 21
N_TILE = 3


def pick(table, index):
    return sum(jnp.where(index == k, v, 0) for k, v in enumerate(table))


def split(value):
    high = value.astype(BF16)
    return high, (value - high.astype(F32)).astype(BF16)


def contract(left, right):
    return lax.dot_general(
        left, right, (((1,), (1,)), ((), ())), preferred_element_type=F32
    )


def three(left_hi, left_lo, right_hi, right_lo):
    result = contract(left_hi, right_hi)
    result += contract(left_hi, right_lo)
    result += contract(left_lo, right_hi)
    return result


def fill_right(cols, right_hi, right_lo, h, xs):
    bands, width = cols.shape[2:]

    def fill(i, carry):
        hi, lo = split(cols[h, pl.ds(16 * xs + 2 * i, 2)].reshape(2 * bands, width))
        to = pl.ds(pl.multiple_of(i * 2 * bands, 16), 2 * bands)
        right_hi[to, :] = hi
        right_lo[to, :] = lo
        return carry

    lax.fori_loop(0, 8, fill, 0)


def kernel(
    pairs, coulomb, left_hi, left_lo, right_hi, right_lo, total,
    cols, rows, scales,
    col_send, col_recv, row_send, row_recv, sub_send, sub_recv, own_sem,
):
    row, col, half = lax.axis_index("row"), lax.axis_index("col"), lax.axis_index("ga")
    x, y, core = row // 4, col // 2, col % 2
    z = 2 * (row % 4) + half
    other = 1 - half
    width = pairs.shape[2]
    quarter = width // NY
    bands = pairs.shape[1]
    n_row = 16

    def place(xx, zz, cc=None):
        return {"row": 4 * xx + zz // 2, "col": col if cc is None else cc, "ga": zz % 2}

    def near(step):
        return place((x + step[0] + NX) % NX, (z + step[1] + NZ) % NZ)

    y_up = {"row": row, "col": (col + 2) % 8, "ga": half}
    y_down = {"row": row, "col": (col + 6) % 8, "ga": half}
    twin = {"row": row, "col": 2 * y + 1 - core, "ga": half}
    pair = {"row": row, "col": col, "ga": other}
    z_out = near((0, 1)), near((0, -1))

    def remote(src, dst, send, recv, device):
        return pltpu.make_async_remote_copy(
            src_ref=src, dst_ref=dst, send_sem=send, recv_sem=recv,
            device_id=device, device_id_type=MESH,
        )

    barrier = pltpu.get_barrier_semaphore()
    for step in range(1, n_row):
        pl.semaphore_signal(
            barrier, inc=1, device_id={"row": (row + step) % n_row, "col": col, "ga": half},
            device_id_type=MESH,
        )
    for device in (*z_out, y_up, y_down, twin):
        pl.semaphore_signal(barrier, inc=1, device_id=device, device_id_type=MESH)

    lanes = pl.ds(pl.multiple_of(y * quarter, 128), quarter)
    own_rows = pltpu.make_async_copy(
        pairs.at[row + 16 * core, :, lanes], rows.at[half, y, core, row], own_sem.at[0]
    )
    own_rows.start()
    per_row = 2.0 * coulomb[...].reshape(1, width) / F32(pairs.shape[0] * n_row)
    scales[half] = jnp.broadcast_to(per_row, (8, width))
    own_cols = []
    for piece in range(4):
        own_cols.append(pltpu.make_async_copy(
            pairs.at[col + 8 * piece], cols.at[half, 4 * row + piece], own_sem.at[2 + piece]
        ))
        own_cols[-1].start()

    pl.semaphore_wait(barrier, n_row - 1 + 5)

    sends = []

    def go(copy):
        copy.start()
        sends.append(copy)

    for step in range(1, n_row):
        to = (row + step) % n_row
        go(remote(
            pairs.at[to + 16 * core, :, lanes], rows.at[half, y, core, row],
            row_send.at[step], row_recv.at[step], {"row": to, "col": col, "ga": half},
        ))

    def slot(code, step=(0, 0)):
        xs = (x + code // 32 - step[0] + NX) % NX
        zs = (z + (code // 4) % 8 - step[1] + NZ) % NZ
        return zs % 2, 4 * (4 * xs + zs // 2) + code % 4

    def send_round(number):
        for way, code in enumerate(PLAN[number]):
            if code < 0:
                continue
            where = cols.at[slot(code)]
            src = pairs.at[col + 8 * (code % 4)] if code < 4 else where
            index = 4 * number + way
            go(remote(src, where, col_send.at[index], col_recv.at[index], near(STEPS[way])))

    def wait_round(number):
        for way, code in enumerate(PLAN[number]):
            if code < 0:
                continue
            where = cols.at[slot(code, STEPS[way])]
            index = 4 * number + way
            remote(
                where, where, col_send.at[index], col_recv.at[index], near(STEPS[way])
            ).wait_recv()

    def part(h, yy, cc):
        return rows.at[h, (yy + NY) % NY, cc]

    def send_part(h, yy, number, device):
        ref = part(h, yy, core)
        go(remote(ref, ref, sub_send.at[number], sub_recv.at[number], device))

    def wait_part(h, yy, cc, number):
        ref = part(h, yy, cc)
        remote(ref, ref, sub_send.at[number], sub_recv.at[number], twin).wait_recv()

    def to_twin(h, yy, number):
        send_part(h, yy, number, twin)

    def exchange(number):
        if number == AT_ROWS:
            own_rows.wait()
            for step in range(1, n_row):
                where = rows.at[half, y, core, (row + n_row - step) % n_row]
                remote(
                    where, where, row_send.at[step], row_recv.at[step], pair
                ).wait_recv()
            go(remote(
                scales.at[half], scales.at[half], sub_send.at[0], sub_recv.at[0], pair
            ))
            send_part(half, y, 1, pair)
            send_part(half, y, 2, y_up)
            send_part(half, y, 3, y_down)
            to_twin(half, y, 8)
        if number == AT_PAIR:
            wait_part(other, y, core, 1)
            send_part(other, y, 4, y_up)
            send_part(other, y, 5, y_down)
            to_twin(other, y, 9)
        if number == AT_FIRST:
            wait_part(half, y - 1, core, 2)
            send_part(half, y - 1, 6, y_up)
            to_twin(half, y - 1, 10)
            wait_part(half, y + 1, core, 3)
            to_twin(half, y + 1, 11)
        if number == AT_SECOND:
            wait_part(other, y + 1, core, 5)
            send_part(other, y + 1, 7, y_down)
            to_twin(other, y + 1, 12)
            wait_part(other, y - 1, core, 4)
            to_twin(other, y - 1, 13)
        if number == AT_RELAY:
            wait_part(half, y - 2, core, 6)
            to_twin(half, y - 2, 14)
            wait_part(other, y + 2, core, 7)
            to_twin(other, y + 2, 15)
        if number == AT_CORE:
            remote(
                scales.at[other], scales.at[other], sub_send.at[0], sub_recv.at[0], pair
            ).wait_recv()
            for n, (h, yy) in enumerate((
                (half, y), (other, y), (half, y - 1), (half, y + 1),
                (other, y + 1), (other, y - 1), (half, y - 2), (other, y + 2),
            )):
                wait_part(h, yy, 1 - core, 8 + n)

            def fill(i, carry):
                h, yy, r = i // (NY * n_row), (i // n_row) % NY, i % n_row
                at = pl.ds(pl.multiple_of(yy * quarter, 128), quarter)
                both = jnp.concatenate([rows[h, yy, 0, r], rows[h, yy, 1, r]], axis=0)
                hi, lo = split(both * scales[h, 0:1, at])
                to = pl.ds(pl.multiple_of(r * 2 * bands, 16), 2 * bands)
                left_hi[h, to, at] = hi
                left_lo[h, to, at] = lo
                return carry

            lax.fori_loop(0, 2 * NY * n_row, fill, 0)

    def tile(u, carry):
        number, m_tile = u // N_TILE, u % N_TILE
        xs = (x + pick([ox for ox, _ in PARTS], number)) % NX
        h = (half + pick([oz for _, oz in PARTS], number)) % 2

        @pl.when(m_tile == 0)
        def _():
            fill_right(cols, right_hi, right_lo, h, xs)

        m = pl.ds(pl.multiple_of(m_tile * M_TILE, M_TILE), M_TILE)
        result = three(left_hi[h, m, :], left_lo[h, m, :], right_hi[...], right_lo[...])
        opens = pick(OPENS, number)

        @pl.when(opens == 1)
        def _():
            total[xs, m, :] = result

        @pl.when(opens == 0)
        def _():
            total[xs, m, :] += result

        return carry

    rounds = len(PLAN)
    done = 0
    for number in range(rounds):
        if number >= LAG:
            wait_round(number - LAG)
        send_round(number)
        exchange(number)
        count = TILES.get(number, 0)
        if count:
            if done == 0:
                for copy in own_cols:
                    copy.wait()
            lax.fori_loop(done, done + count, tile, 0)
            done += count
    for number in range(rounds - LAG, rounds - 1):
        wait_round(number)
    lax.fori_loop(done, EARLY, tile, 0)
    wait_round(rounds - 1)
    ox, oz = PARTS[-1]
    fill_right(cols, right_hi, right_lo, (half + oz) % 2, (x + ox) % NX)
    for copy in sends:
        copy.wait_send()


def last_kernel(left_hi, left_lo, right_hi, right_lo, total, out, result, sems):
    row, half = lax.axis_index("row"), lax.axis_index("ga")
    ox, oz = PARTS[-1]
    xs, h = (row // 4 + ox) % NX, (half + oz) % 2
    group = result.shape[2]

    def lanes(k):
        return pl.ds(pl.multiple_of(((xs + k) % NX) * group, 128), group)

    others = []
    for k in range(1, NX):
        others.append(pltpu.make_async_copy(
            total.at[(xs + k) % NX], out.at[:, lanes(k)], sems.at[N_TILE + k - 1]
        ))
        others[-1].start()

    def part(m_tile):
        m = pl.ds(pl.multiple_of(m_tile * M_TILE, M_TILE), M_TILE)
        return m, pltpu.make_async_copy(
            result.at[m_tile], out.at[m, lanes(0)], sems.at[m_tile]
        )

    def tile(m_tile, carry):
        m, copy = part(m_tile)
        result[m_tile] = total[xs, m, :] + three(
            left_hi[h, m, :], left_lo[h, m, :], right_hi[...], right_lo[...]
        )
        copy.start()
        return carry

    lax.fori_loop(0, N_TILE, tile, 0)
    for m_tile in range(N_TILE):
        part(m_tile)[1].wait()
    for copy in others:
        copy.wait()


def local(pair_density, coulomb):
    local_k, bands, width = pair_density.shape
    n_row = lax.axis_size("row")
    m = 2 * n_row * bands
    n = 4 * n_row * bands
    group = n // NX
    rounds = len(PLAN)
    passed = pl.pallas_call(
        kernel,
        out_shape=[
            pltpu.VMEM((2, m, width), BF16),
            pltpu.VMEM((2, m, width), BF16),
            pltpu.VMEM((group, width), BF16),
            pltpu.VMEM((group, width), BF16),
            pltpu.VMEM((NX, m, group), F32),
        ],
        in_specs=[pl.BlockSpec(memory_space=pl.ANY), pl.BlockSpec(memory_space=pltpu.VMEM)],
        out_specs=[pl.BlockSpec(memory_space=pltpu.VMEM)] * 5,
        scratch_shapes=[
            pltpu.VMEM((2, 4 * n_row, bands, width), F32),
            pltpu.VMEM((2, NY, 2, n_row, bands, width // NY), F32),
            pltpu.VMEM((2, 8, width), F32),
            pltpu.SemaphoreType.DMA((4 * rounds,)),
            pltpu.SemaphoreType.DMA((4 * rounds,)),
            pltpu.SemaphoreType.DMA((n_row,)),
            pltpu.SemaphoreType.DMA((n_row,)),
            pltpu.SemaphoreType.DMA((16,)),
            pltpu.SemaphoreType.DMA((16,)),
            pltpu.SemaphoreType.DMA((6,)),
        ],
        compiler_params=pltpu.CompilerParams(
            collective_id=0, has_side_effects=True, vmem_limit_bytes=FIRST_LIMIT
        ),
        name="gather_and_contract",
    )(pair_density, coulomb)
    return pl.pallas_call(
        last_kernel,
        out_shape=jax.ShapeDtypeStruct((m, n), F32),
        in_specs=[pl.BlockSpec(memory_space=pltpu.VMEM)] * 5,
        out_specs=pl.BlockSpec(memory_space=pl.ANY),
        scratch_shapes=[
            pltpu.VMEM((N_TILE, M_TILE, group), F32),
            pltpu.SemaphoreType.DMA((N_TILE + NX - 1,)),
        ],
        compiler_params=pltpu.CompilerParams(vmem_limit_bytes=LAST_LIMIT),
        name="contract_last",
    )(*passed)


def solution(mesh):
    placed = (P("row", None, "ga"), P("ga"))
    return jax.shard_map(
        local, mesh=mesh, in_specs=placed, out_specs=P("row", "col"), check_vma=False
    )
```

```python
import jax
import jax.numpy as jnp
from jax import lax
from jax.experimental import pallas as pl
from jax.experimental.pallas import tpu as pltpu
from jax.sharding import PartitionSpec as P

MESH = pl.DeviceIdType.MESH
F32 = jnp.float32
BF16 = jnp.bfloat16

LAG = 3
PLAN = (
    (1, 1, 2, 2),
    (0, 0, 1, 3),
    (-1, -1, 0, 1),
    (28, 28, 28, 0),
    (4, 5, -1, -1),
    (5, 4, 31, 4),
    (96, 33, 30, 7),
    (100, 37, 3, 5),
    (25, 25, 25, 10),
    (24, 24, -1, -1),
    (9, 9, 26, 11),
    (29, 29, 29, 6),
    (12, 12, 24, 9),
    (20, 20, 23, 13),
    (8, 8, 27, 12),
    (13, 13, 22, 8),
    (17, 17, -1, -1),
    (21, 21, -1, -1),
    (16, 16, -1, -1),
    (121, 61, -1, -1),
    (105, 40, -1, -1),
    (117, 60, -1, -1),
    (109, 44, -1, -1),
    (120, 52, -1, -1),
    (113, 48, -1, -1),
)
STEPS = ((1, 0), (-1, 0), (0, 1), (0, -1))
NX, NZ, NY = 4, 8, 4
M_TILE = 256
FIRST_LIMIT, LAST_LIMIT = 48 * 2**20, 6 * 2**20

CHUNKS = (0, 1, 3, 2)
SEND = (0, 1, 3, 5)
ROWS, PAIR, FIRST, SECOND, RELAY, CORE = 3, 6, 6, 8, 10, 12
SHARED = (1, 3, 2)
N_TILE = 3
CATCH_UP = 19
TILES = {20: 1, 21: 1, 22: 1, 23: 2, 24: 1}


def split(value):
    high = value.astype(BF16)
    return high, (value - high.astype(F32)).astype(BF16)


def contract(left, right):
    return lax.dot_general(
        left, right, (((1,), (1,)), ((), ())), preferred_element_type=F32
    )


def three(left_hi, left_lo, right_hi, right_lo):
    result = contract(left_hi, right_hi)
    result += contract(left_hi, right_lo)
    result += contract(left_lo, right_hi)
    return result


def fill_right(cols, right_hi, right_lo, first, count):
    bands, width = cols.shape[2:]

    def fill(i, carry):
        h, n = i // count, i % count
        hi, lo = split(cols[h, pl.ds(first(n), 2)].reshape(2 * bands, width))
        to = pl.ds(pl.multiple_of(n * 2 * bands, 16), 2 * bands)
        at = pl.ds(pl.multiple_of(h * width, 128), width)
        right_hi[to, at] = hi
        right_lo[to, at] = lo
        return carry

    lax.fori_loop(0, 2 * count, fill, 0)


def merge(shared, total, index, m_tile, xs):
    lane = lax.broadcasted_iota(jnp.int32, (64, 384), 1)
    run = lane // 48
    for i in range(4):
        wide = []
        for owner in range(2):
            one = shared[owner, index, m_tile, 64 * i : 64 * i + 64, :]
            at = 256 + 64 * (i % 2)
            two = shared[owner, index, m_tile, at : at + 64, :]
            if i // 2:
                two = pltpu.roll(two, 64, 1)
            wide.append(jnp.concatenate([one, two, two], axis=1))
        value = wide[0]
        for k in range(1, 8):
            turned = pltpu.roll(wide[k % 2], 48 * ((k + 1) // 2), 1)
            value = jnp.where(run == k, turned, value)
        m = pl.ds(pl.multiple_of(m_tile * M_TILE, M_TILE) + 64 * i, 64)
        total[xs, m, :] = value


def kernel(
    pairs, coulomb, total, shared,
    cols, rows, scales, left_hi, left_lo, right_hi, right_lo,
    col_send, col_recv, row_send, row_recv, sub_send, sub_recv, out_send, out_recv, own_sem,
):
    row, col, half = lax.axis_index("row"), lax.axis_index("col"), lax.axis_index("ga")
    x, y, core = row // 4, col // 2, col % 2
    z = 2 * (row % 4) + half
    other = 1 - half
    width = pairs.shape[2]
    quarter = width // NY
    bands = pairs.shape[1]
    n_row = 16

    def place(xx, zz, cc=None):
        return {"row": 4 * xx + zz // 2, "col": col if cc is None else cc, "ga": zz % 2}

    def near(step):
        return place((x + step[0] + NX) % NX, (z + step[1] + NZ) % NZ)

    y_up = {"row": row, "col": (col + 2) % 8, "ga": half}
    y_down = {"row": row, "col": (col + 6) % 8, "ga": half}
    twin = {"row": row, "col": 2 * y + 1 - core, "ga": half}
    pair = {"row": row, "col": col, "ga": other}

    def remote(src, dst, send, recv, device):
        return pltpu.make_async_remote_copy(
            src_ref=src, dst_ref=dst, send_sem=send, recv_sem=recv,
            device_id=device, device_id_type=MESH,
        )

    zh = row % 4
    sign = 2 * half - 1

    def at_row(xx, zz):
        return 4 * ((xx + NX) % NX) + (zz + 4) % 4

    barrier = pltpu.get_barrier_semaphore()
    peers = [(at_row(x + dx, zh + dz), half) for dx in range(NX) for dz in (-1, 0, 1) if dx or dz]
    peers += [(at_row(x + dx, zh + dz * sign), other) for dx in range(NX) for dz in (1, 2)]
    peers = [{"row": r, "col": col, "ga": g} for r, g in peers] + [pair, y_up, y_down, twin]
    for device in peers:
        pl.semaphore_signal(barrier, inc=1, device_id=device, device_id_type=MESH)

    lanes = pl.ds(pl.multiple_of(y * quarter, 128), quarter)
    own_rows = pltpu.make_async_copy(
        pairs.at[row + 16 * core, :, lanes], rows.at[half, y, core, 4 * x], own_sem.at[0]
    )
    own_rows.start()
    per_row = 2.0 * coulomb[...].reshape(1, width) / F32(pairs.shape[0] * n_row)
    scales[half] = jnp.broadcast_to(per_row, (8, width))
    own_cols = []
    for piece in range(4):
        own_cols.append(pltpu.make_async_copy(
            pairs.at[col + 8 * piece], cols.at[half, 4 * row + piece], own_sem.at[2 + piece]
        ))
        own_cols[-1].start()

    pl.semaphore_wait(barrier, len(peers))

    sends = []

    def go(copy):
        copy.start()
        sends.append(copy)

    def slot(code, step=(0, 0)):
        xs = (x + code // 32 - step[0] + NX) % NX
        zs = (z + (code // 4) % 8 - step[1] + NZ) % NZ
        piece = (2 * half + 2 * (step[1] != 0) + code % 4) % 4
        return zs % 2, 4 * (4 * xs + zs // 2) + piece

    def send_round(number):
        for way, code in enumerate(PLAN[number]):
            if code < 0:
                continue
            where = cols.at[slot(code)]
            src = pairs.at[col + 8 * ((2 * half + code) % 4)] if code < 4 else where
            index = 4 * number + way
            go(remote(src, where, col_send.at[index], col_recv.at[index], near(STEPS[way])))

    def wait_round(number):
        for way, code in enumerate(PLAN[number]):
            if code < 0:
                continue
            where = cols.at[slot(code, STEPS[way])]
            index = 4 * number + way
            remote(
                where, where, col_send.at[index], col_recv.at[index], near(STEPS[way])
            ).wait_recv()

    def part(i, h, yy, cc):
        xs = (x + CHUNKS[i]) % NX
        return rows.at[h, (yy + NY) % NY, cc, pl.ds(4 * xs, 4)]

    def send_part(i, h, yy, number, device):
        ref, at = part(i, h, yy, core), 16 * i + number
        go(remote(ref, ref, sub_send.at[at], sub_recv.at[at], device))

    def wait_part(i, h, yy, cc, number):
        ref, at = part(i, h, yy, cc), 16 * i + number
        remote(ref, ref, sub_send.at[at], sub_recv.at[at], twin).wait_recv()

    def to_twin(i, h, yy, number):
        send_part(i, h, yy, number, twin)

    ways = ((0, 1, 0), (-sign, 1, 1), (sign, 0, 2), (2 * sign, 0, 3))

    def exchange(number):
        for i in range(NX):
            after = number - SEND[i]
            if after == 0:
                for step, same, place_no in ways:
                    if not CHUNKS[i] and place_no == 0:
                        continue
                    to, at = at_row(x - CHUNKS[i], zh + step), 4 * CHUNKS[i] + place_no
                    ga = half if same else other
                    go(remote(
                        pairs.at[to + 16 * core, :, lanes],
                        rows.at[ga, y, core, 4 * x + place_no],
                        row_send.at[at], row_recv.at[at], {"row": to, "col": col, "ga": ga},
                    ))
            if after == ROWS:
                if not CHUNKS[i]:
                    own_rows.wait()
                    go(remote(
                        scales.at[half], scales.at[half], sub_send.at[0], sub_recv.at[0], pair
                    ))
                for place_no in range(4):
                    if not CHUNKS[i] and place_no == 0:
                        continue
                    at = 4 * CHUNKS[i] + place_no
                    where = rows.at[half, y, core, at_row(x + CHUNKS[i], 0) + place_no]
                    remote(where, where, row_send.at[at], row_recv.at[at], pair).wait_recv()
                send_part(i, half, y, 1, pair)
                send_part(i, half, y, 2, y_up)
                send_part(i, half, y, 3, y_down)
                to_twin(i, half, y, 8)
            if after == FIRST:
                wait_part(i, half, y - 1, core, 2)
                send_part(i, half, y - 1, 6, y_up)
                to_twin(i, half, y - 1, 10)
                wait_part(i, half, y + 1, core, 3)
                to_twin(i, half, y + 1, 11)
            if after == PAIR:
                wait_part(i, other, y, core, 1)
                send_part(i, other, y, 4, y_up)
                send_part(i, other, y, 5, y_down)
                to_twin(i, other, y, 9)
            if after == SECOND:
                wait_part(i, other, y + 1, core, 5)
                send_part(i, other, y + 1, 7, y_down)
                to_twin(i, other, y + 1, 12)
                wait_part(i, other, y - 1, core, 4)
                to_twin(i, other, y - 1, 13)
            if after == RELAY:
                wait_part(i, half, y - 2, core, 6)
                to_twin(i, half, y - 2, 14)
                wait_part(i, other, y + 2, core, 7)
                to_twin(i, other, y + 2, 15)
            if after == CORE:
                if not CHUNKS[i]:
                    remote(
                        scales.at[other], scales.at[other], sub_send.at[0], sub_recv.at[0], pair
                    ).wait_recv()
                for n, (h, yy) in enumerate((
                    (half, y), (other, y), (half, y - 1), (half, y + 1),
                    (other, y + 1), (other, y - 1), (half, y - 2), (other, y + 2),
                )):
                    wait_part(i, h, yy, 1 - core, 8 + n)
                fill_left(at_row(x + CHUNKS[i], 0))

    def fill_left(first):
        def fill(i, carry):
            o, yy, n = i // (NY * 4), (i // 4) % NY, i % 4
            h = (o + n // 2) % 2
            r = first + (zh + 4 + (2 * o - 1) * ((n + 1) // 2)) % 4
            at = pl.ds(pl.multiple_of(yy * quarter, 128), quarter)
            both = jnp.concatenate([rows[o, yy, 0, first + n], rows[o, yy, 1, first + n]], axis=0)
            hi, lo = split(both * scales[h, 0:1, at])
            to = pl.ds(pl.multiple_of(r * 2 * bands, 16), 2 * bands)
            at = pl.ds(pl.multiple_of(h * width + yy * quarter, 128), quarter)
            left_hi[to, at] = hi
            left_lo[to, at] = lo
            return carry

        lax.fori_loop(0, 2 * NY * 4, fill, 0)

    def rows_of(m_tile):
        return pl.ds(pl.multiple_of(m_tile * M_TILE, M_TILE), M_TILE)

    def swap(index, m_tile, owner):
        ref = shared.at[owner, index, m_tile]
        at = N_TILE * index + m_tile
        return remote(ref, ref, out_send.at[at], out_recv.at[at], pair)

    def shared_tile(number):
        index, m_tile = number // N_TILE, number % N_TILE
        if m_tile == 0:
            xs = (x + SHARED[index]) % NX
            fill_right(
                cols, right_hi, right_lo, lambda n: 4 * (4 * xs + n) + 2 * half, 4
            )
        m = rows_of(m_tile)
        result = three(
            left_hi[m, :], left_lo[m, :], right_hi[0:256, :], right_lo[0:256, :]
        )
        shared[half, index, m_tile, 0:256, :] = result[:, :128]
        shared[half, index, m_tile, 256:384, :] = result[:128, 128:] + pltpu.roll(
            result[128:, 128:], 64, 1
        )

    def merge_tile(index, m_tile):
        swap(index, m_tile, other).wait_recv()
        merge(shared, total, index, m_tile, (x + SHARED[index]) % NX)

    def merge_offset(index, count):
        def one(m_tile, carry):
            merge_tile(index, m_tile)
            return carry

        lax.fori_loop(0, count, one, 0)

    rounds = len(PLAN)
    zero = jnp.zeros((256 - 8 * bands, 2 * width), BF16)
    right_hi[8 * bands : 256, :] = zero
    right_lo[8 * bands : 256, :] = zero
    waited = sent = done = 0
    for number in range(rounds):
        while waited <= number - (2 if number >= CATCH_UP else LAG):
            wait_round(waited)
            waited += 1
        send_round(number)
        if sent < done:
            swap(sent // N_TILE, sent % N_TILE, half).start()
            sent += 1
        exchange(number)
        for _ in range(TILES.get(number, 0)):
            shared_tile(done)
            done += 1
            if sent < done - 1:
                swap(sent // N_TILE, sent % N_TILE, half).start()
                sent += 1
    for number in range(waited, rounds):
        wait_round(number)
    while done < 3 * N_TILE:
        shared_tile(done)
        done += 1
        swap(sent // N_TILE, sent % N_TILE, half).start()
        sent += 1
    for copy in own_cols:
        copy.wait()
    swap(sent // N_TILE, sent % N_TILE, half).start()
    merge_offset(0, N_TILE)
    fill_right(cols, right_hi, right_lo, lambda n: 16 * x + 2 * n, 8)

    def own_tile(m_tile, carry):
        m = rows_of(m_tile)
        total[x, m, :] = three(left_hi[m, :], left_lo[m, :], right_hi[...], right_lo[...])
        return carry

    lax.fori_loop(0, N_TILE, own_tile, 0)
    merge_offset(1, N_TILE)
    merge_offset(2, N_TILE - 1)
    for copy in sends:
        copy.wait_send()
    for index in range(3):
        for m_tile in range(N_TILE):
            swap(index, m_tile, half).wait_send()
    swap(2, N_TILE - 1, other).wait_recv()


def last_kernel(total, shared, out, result, sems):
    x = lax.axis_index("row") // 4
    group = total.shape[2]

    def lanes(xs):
        return pl.ds(pl.multiple_of(xs * group, 128), group)

    copies = []
    for k in range(NX):
        xs = (x + k) % NX
        for part in range(2):
            m = pl.ds(512 * part, 512 if part == 0 else 256)
            if k == SHARED[2] and part == 1:
                merge(shared, result, 2, N_TILE - 1, 0)
                src = result.at[0, m]
            else:
                src = total.at[xs, m]
            copies.append(pltpu.make_async_copy(
                src, out.at[m, lanes(xs)], sems.at[2 * k + part]
            ))
    last = 2 * SHARED[2] + 1
    for k, copy in enumerate(copies):
        if k != last:
            copy.start()
    copies[last].start()
    for copy in copies:
        copy.wait()


def local(pair_density, coulomb):
    local_k, bands, width = pair_density.shape
    n_row = lax.axis_size("row")
    m = 2 * n_row * bands
    n = 4 * n_row * bands
    group = n // NX
    rounds = len(PLAN)
    passed = pl.pallas_call(
        kernel,
        out_shape=[
            pltpu.VMEM((NX, m, group), F32),
            pltpu.VMEM((2, len(SHARED), N_TILE, m // 2, 128), F32),
        ],
        in_specs=[pl.BlockSpec(memory_space=pl.ANY), pl.BlockSpec(memory_space=pltpu.VMEM)],
        out_specs=[pl.BlockSpec(memory_space=pltpu.VMEM)] * 2,
        scratch_shapes=[
            pltpu.VMEM((2, 4 * n_row, bands, width), F32),
            pltpu.VMEM((2, NY, 2, n_row, bands, width // NY), F32),
            pltpu.VMEM((2, 8, width), F32),
            pltpu.VMEM((m, 2 * width), BF16),
            pltpu.VMEM((m, 2 * width), BF16),
            pltpu.VMEM((group, 2 * width), BF16),
            pltpu.VMEM((group, 2 * width), BF16),
            pltpu.SemaphoreType.DMA((4 * rounds,)),
            pltpu.SemaphoreType.DMA((4 * rounds,)),
            pltpu.SemaphoreType.DMA((n_row,)),
            pltpu.SemaphoreType.DMA((n_row,)),
            pltpu.SemaphoreType.DMA((64,)),
            pltpu.SemaphoreType.DMA((64,)),
            pltpu.SemaphoreType.DMA((3 * N_TILE,)),
            pltpu.SemaphoreType.DMA((3 * N_TILE,)),
            pltpu.SemaphoreType.DMA((6,)),
        ],
        compiler_params=pltpu.CompilerParams(
            collective_id=0, has_side_effects=True, vmem_limit_bytes=FIRST_LIMIT
        ),
        name="gather_and_contract",
    )(pair_density, coulomb)
    return pl.pallas_call(
        last_kernel,
        out_shape=jax.ShapeDtypeStruct((m, n), F32),
        in_specs=[pl.BlockSpec(memory_space=pltpu.VMEM)] * 2,
        out_specs=pl.BlockSpec(memory_space=pl.ANY),
        scratch_shapes=[
            pltpu.VMEM((1, m, group), F32),
            pltpu.SemaphoreType.DMA((2 * NX,)),
        ],
        compiler_params=pltpu.CompilerParams(vmem_limit_bytes=LAST_LIMIT),
        name="write_result",
    )(*passed)


def solution(mesh):
    placed = (P("row", None, "ga"), P("ga"))
    return jax.shard_map(
        local, mesh=mesh, in_specs=placed, out_specs=P("row", "col"), check_vma=False
    )
```

```python
import jax
import jax.numpy as jnp
from jax import lax
from jax.experimental import pallas as pl
from jax.experimental.pallas import tpu as pltpu
from jax.sharding import PartitionSpec as P

MESH = pl.DeviceIdType.MESH
F32 = jnp.float32
BF16 = jnp.bfloat16

LAG = 3
PLAN = (
    (1, 1, 2, 2),
    (0, 0, 1, 3),
    (-1, -1, 0, 1),
    (28, 28, 28, 0),
    (4, 5, -1, -1),
    (5, 4, 31, 4),
    (96, 33, 30, 7),
    (100, 37, 3, 5),
    (25, 25, 25, 10),
    (24, 24, -1, -1),
    (9, 9, 26, 11),
    (29, 29, 29, 6),
    (12, 12, 24, 9),
    (20, 20, 23, 13),
    (8, 8, 27, 12),
    (13, 13, 22, 8),
    (17, 17, -1, -1),
    (21, 21, -1, -1),
    (16, 16, -1, -1),
    (121, 61, -1, -1),
    (105, 40, -1, -1),
    (117, 60, -1, -1),
    (109, 44, -1, -1),
    (120, 52, -1, -1),
    (113, 48, -1, -1),
)
STEPS = ((1, 0), (-1, 0), (0, 1), (0, -1))
NX, NZ, NY = 4, 8, 4
M_TILE = 256
FIRST_LIMIT, LAST_LIMIT = 48 * 2**20, 6 * 2**20

CHUNKS = (0, 1, 3, 2)
SEND = (1, 3, 5, 7)
ROWS, PAIR, FIRST, SECOND, RELAY, CORE = 3, 6, 6, 8, 10, 12
SHARED = (1, 3, 2)
N_TILE = 3
CATCH_UP = 19
TILES = {20: 1, 21: 1, 22: 1, 23: 2, 24: 1}


def split(value):
    high = value.astype(BF16)
    return high, (value - high.astype(F32)).astype(BF16)


def contract(left, right):
    return lax.dot_general(
        left, right, (((1,), (1,)), ((), ())), preferred_element_type=F32
    )


def three(left_hi, left_lo, right_hi, right_lo):
    result = contract(left_hi, right_hi)
    result += contract(left_hi, right_lo)
    result += contract(left_lo, right_hi)
    return result


def fill_right(cols, right_hi, right_lo, first, count):
    bands, width = cols.shape[2:]

    def fill(i, carry):
        h, n = i // count, i % count
        hi, lo = split(cols[h, pl.ds(first(n), 2)].reshape(2 * bands, width))
        to = pl.ds(pl.multiple_of(n * 2 * bands, 16), 2 * bands)
        at = pl.ds(pl.multiple_of(h * width, 128), width)
        right_hi[to, at] = hi
        right_lo[to, at] = lo
        return carry

    lax.fori_loop(0, 2 * count, fill, 0)


def merge(shared, total, index, m_tile, xs):
    lane = lax.broadcasted_iota(jnp.int32, (64, 384), 1)
    run = lane // 48
    for i in range(4):
        wide = []
        for owner in range(2):
            one = shared[owner, index, m_tile, 64 * i : 64 * i + 64, :]
            at = 256 + 64 * (i % 2)
            two = shared[owner, index, m_tile, at : at + 64, :]
            if i // 2:
                two = pltpu.roll(two, 64, 1)
            wide.append(jnp.concatenate([one, two, two], axis=1))
        value = wide[0]
        for k in range(1, 8):
            turned = pltpu.roll(wide[k % 2], 48 * ((k + 1) // 2), 1)
            value = jnp.where(run == k, turned, value)
        m = pl.ds(pl.multiple_of(m_tile * M_TILE, M_TILE) + 64 * i, 64)
        total[xs, m, :] = value


def kernel(
    pairs, coulomb, total, shared,
    cols, rows, scales, left_hi, left_lo, right_hi, right_lo,
    col_send, col_recv, row_send, row_recv, sub_send, sub_recv, out_send, out_recv, own_sem,
):
    row, col, half = lax.axis_index("row"), lax.axis_index("col"), lax.axis_index("ga")
    x, y, core = row // 4, col // 2, col % 2
    z = 2 * (row % 4) + half
    other = 1 - half
    width = pairs.shape[2]
    quarter = width // NY
    bands = pairs.shape[1]
    n_row = 16

    def place(xx, zz, cc=None):
        return {"row": 4 * xx + zz // 2, "col": col if cc is None else cc, "ga": zz % 2}

    def near(step):
        return place((x + step[0] + NX) % NX, (z + step[1] + NZ) % NZ)

    y_up = {"row": row, "col": (col + 2) % 8, "ga": half}
    y_down = {"row": row, "col": (col + 6) % 8, "ga": half}
    twin = {"row": row, "col": 2 * y + 1 - core, "ga": half}
    pair = {"row": row, "col": col, "ga": other}

    def remote(src, dst, send, recv, device):
        return pltpu.make_async_remote_copy(
            src_ref=src, dst_ref=dst, send_sem=send, recv_sem=recv,
            device_id=device, device_id_type=MESH,
        )

    zh = row % 4
    sign = 2 * half - 1

    def at_row(xx, zz):
        return 4 * ((xx + NX) % NX) + (zz + 4) % 4

    barrier = pltpu.get_barrier_semaphore()
    peers = [(at_row(x + dx, zh + dz), half) for dx in range(NX) for dz in (-1, 0, 1) if dx or dz]
    peers += [(at_row(x + dx, zh + dz * sign), other) for dx in range(NX) for dz in (1, 2)]
    peers = [{"row": r, "col": col, "ga": g} for r, g in peers] + [pair, y_up, y_down, twin]
    for device in peers:
        pl.semaphore_signal(barrier, inc=1, device_id=device, device_id_type=MESH)

    lanes = pl.ds(pl.multiple_of(y * quarter, 128), quarter)
    own_rows = pltpu.make_async_copy(
        pairs.at[row + 16 * core, :, lanes], rows.at[half, y, core, 4 * x], own_sem.at[0]
    )
    own_rows.start()
    per_row = 2.0 * coulomb[...].reshape(1, width) / F32(pairs.shape[0] * n_row)
    scales[half] = jnp.broadcast_to(per_row, (8, width))
    own_cols = []
    for piece in range(4):
        own_cols.append(pltpu.make_async_copy(
            pairs.at[col + 8 * piece], cols.at[half, 4 * row + piece], own_sem.at[2 + piece]
        ))
        own_cols[-1].start()

    pl.semaphore_wait(barrier, len(peers))

    sends = []

    def go(copy):
        copy.start()
        sends.append(copy)

    def slot(code, step=(0, 0)):
        xs = (x + code // 32 - step[0] + NX) % NX
        zs = (z + (code // 4) % 8 - step[1] + NZ) % NZ
        piece = (2 * half + 2 * (step[1] != 0) + code % 4) % 4
        return zs % 2, 4 * (4 * xs + zs // 2) + piece

    def send_round(number):
        for way, code in enumerate(PLAN[number]):
            if code < 0:
                continue
            where = cols.at[slot(code)]
            src = pairs.at[col + 8 * ((2 * half + code) % 4)] if code < 4 else where
            index = 4 * number + way
            go(remote(src, where, col_send.at[index], col_recv.at[index], near(STEPS[way])))

    def wait_round(number):
        for way, code in enumerate(PLAN[number]):
            if code < 0:
                continue
            where = cols.at[slot(code, STEPS[way])]
            index = 4 * number + way
            remote(
                where, where, col_send.at[index], col_recv.at[index], near(STEPS[way])
            ).wait_recv()

    def part(i, h, yy, cc):
        xs = (x + CHUNKS[i]) % NX
        return rows.at[h, (yy + NY) % NY, cc, pl.ds(4 * xs, 4)]

    def send_part(i, h, yy, number, device):
        ref, at = part(i, h, yy, core), 16 * i + number
        go(remote(ref, ref, sub_send.at[at], sub_recv.at[at], device))

    def wait_part(i, h, yy, cc, number):
        ref, at = part(i, h, yy, cc), 16 * i + number
        remote(ref, ref, sub_send.at[at], sub_recv.at[at], twin).wait_recv()

    def to_twin(i, h, yy, number):
        send_part(i, h, yy, number, twin)

    ways = ((0, 1, 0), (-sign, 1, 1), (sign, 0, 2), (2 * sign, 0, 3))

    def exchange(number):
        for i in range(NX):
            after = number - SEND[i]
            if after == 0:
                for step, same, place_no in ways:
                    if not CHUNKS[i] and place_no == 0:
                        continue
                    to, at = at_row(x - CHUNKS[i], zh + step), 4 * CHUNKS[i] + place_no
                    ga = half if same else other
                    go(remote(
                        pairs.at[to + 16 * core, :, lanes],
                        rows.at[ga, y, core, 4 * x + place_no],
                        row_send.at[at], row_recv.at[at], {"row": to, "col": col, "ga": ga},
                    ))
            if after == ROWS:
                if not CHUNKS[i]:
                    own_rows.wait()
                    go(remote(
                        scales.at[half], scales.at[half], sub_send.at[0], sub_recv.at[0], pair
                    ))
                for place_no in range(4):
                    if not CHUNKS[i] and place_no == 0:
                        continue
                    at = 4 * CHUNKS[i] + place_no
                    where = rows.at[half, y, core, at_row(x + CHUNKS[i], 0) + place_no]
                    remote(where, where, row_send.at[at], row_recv.at[at], pair).wait_recv()
                send_part(i, half, y, 1, pair)
                send_part(i, half, y, 2, y_up)
                send_part(i, half, y, 3, y_down)
                to_twin(i, half, y, 8)
            if after == FIRST:
                wait_part(i, half, y - 1, core, 2)
                send_part(i, half, y - 1, 6, y_up)
                to_twin(i, half, y - 1, 10)
                wait_part(i, half, y + 1, core, 3)
                to_twin(i, half, y + 1, 11)
            if after == PAIR:
                wait_part(i, other, y, core, 1)
                send_part(i, other, y, 4, y_up)
                send_part(i, other, y, 5, y_down)
                to_twin(i, other, y, 9)
            if after == SECOND:
                wait_part(i, other, y + 1, core, 5)
                send_part(i, other, y + 1, 7, y_down)
                to_twin(i, other, y + 1, 12)
                wait_part(i, other, y - 1, core, 4)
                to_twin(i, other, y - 1, 13)
            if after == RELAY:
                wait_part(i, half, y - 2, core, 6)
                to_twin(i, half, y - 2, 14)
                wait_part(i, other, y + 2, core, 7)
                to_twin(i, other, y + 2, 15)
            if after == CORE:
                if not CHUNKS[i]:
                    remote(
                        scales.at[other], scales.at[other], sub_send.at[0], sub_recv.at[0], pair
                    ).wait_recv()
                for n, (h, yy) in enumerate((
                    (half, y), (other, y), (half, y - 1), (half, y + 1),
                    (other, y + 1), (other, y - 1), (half, y - 2), (other, y + 2),
                )):
                    wait_part(i, h, yy, 1 - core, 8 + n)
                fill_left(at_row(x + CHUNKS[i], 0))

    def fill_left(first):
        def fill(i, carry):
            o, yy, n = i // (NY * 4), (i // 4) % NY, i % 4
            h = (o + n // 2) % 2
            r = first + (zh + 4 + (2 * o - 1) * ((n + 1) // 2)) % 4
            at = pl.ds(pl.multiple_of(yy * quarter, 128), quarter)
            both = jnp.concatenate([rows[o, yy, 0, first + n], rows[o, yy, 1, first + n]], axis=0)
            hi, lo = split(both * scales[h, 0:1, at])
            to = pl.ds(pl.multiple_of(r * 2 * bands, 16), 2 * bands)
            at = pl.ds(pl.multiple_of(h * width + yy * quarter, 128), quarter)
            left_hi[to, at] = hi
            left_lo[to, at] = lo
            return carry

        lax.fori_loop(0, 2 * NY * 4, fill, 0)

    def rows_of(m_tile):
        return pl.ds(pl.multiple_of(m_tile * M_TILE, M_TILE), M_TILE)

    def swap(index, m_tile, owner):
        ref = shared.at[owner, index, m_tile]
        at = N_TILE * index + m_tile
        return remote(ref, ref, out_send.at[at], out_recv.at[at], pair)

    def shared_tile(number):
        index, m_tile = number // N_TILE, number % N_TILE
        if m_tile == 0:
            xs = (x + SHARED[index]) % NX
            fill_right(
                cols, right_hi, right_lo, lambda n: 4 * (4 * xs + n) + 2 * half, 4
            )
        m = rows_of(m_tile)
        result = three(
            left_hi[m, :], left_lo[m, :], right_hi[0:256, :], right_lo[0:256, :]
        )
        shared[half, index, m_tile, 0:256, :] = result[:, :128]
        shared[half, index, m_tile, 256:384, :] = result[:128, 128:] + pltpu.roll(
            result[128:, 128:], 64, 1
        )

    def merge_tile(index, m_tile):
        swap(index, m_tile, other).wait_recv()
        merge(shared, total, index, m_tile, (x + SHARED[index]) % NX)

    def merge_offset(index, count):
        def one(m_tile, carry):
            merge_tile(index, m_tile)
            return carry

        lax.fori_loop(0, count, one, 0)

    rounds = len(PLAN)
    zero = jnp.zeros((256 - 8 * bands, 2 * width), BF16)
    right_hi[8 * bands : 256, :] = zero
    right_lo[8 * bands : 256, :] = zero
    waited = sent = done = 0
    for number in range(rounds):
        while waited <= number - (2 if number >= CATCH_UP else LAG):
            wait_round(waited)
            waited += 1
        send_round(number)
        if sent < done:
            swap(sent // N_TILE, sent % N_TILE, half).start()
            sent += 1
        exchange(number)
        for _ in range(TILES.get(number, 0)):
            shared_tile(done)
            done += 1
            if sent < done - 1:
                swap(sent // N_TILE, sent % N_TILE, half).start()
                sent += 1
    for number in range(waited, rounds):
        wait_round(number)
    while done < 3 * N_TILE:
        shared_tile(done)
        done += 1
        swap(sent // N_TILE, sent % N_TILE, half).start()
        sent += 1
    for copy in own_cols:
        copy.wait()
    swap(sent // N_TILE, sent % N_TILE, half).start()
    merge_offset(0, N_TILE)
    fill_right(cols, right_hi, right_lo, lambda n: 16 * x + 2 * n, 8)

    def own_tile(m_tile, carry):
        m = rows_of(m_tile)
        total[x, m, :] = three(left_hi[m, :], left_lo[m, :], right_hi[...], right_lo[...])
        return carry

    lax.fori_loop(0, N_TILE, own_tile, 0)
    merge_offset(1, N_TILE)
    merge_offset(2, N_TILE - 1)
    for copy in sends:
        copy.wait_send()
    for index in range(3):
        for m_tile in range(N_TILE):
            swap(index, m_tile, half).wait_send()
    swap(2, N_TILE - 1, other).wait_recv()


def last_kernel(total, shared, out, result, sems):
    x = lax.axis_index("row") // 4
    group = total.shape[2]

    def lanes(xs):
        return pl.ds(pl.multiple_of(xs * group, 128), group)

    copies = []
    for k in range(NX):
        xs = (x + k) % NX
        for part in range(2):
            m = pl.ds(512 * part, 512 if part == 0 else 256)
            if k == SHARED[2] and part == 1:
                merge(shared, result, 2, N_TILE - 1, 0)
                src = result.at[0, m]
            else:
                src = total.at[xs, m]
            copies.append(pltpu.make_async_copy(
                src, out.at[m, lanes(xs)], sems.at[2 * k + part]
            ))
    last = 2 * SHARED[2] + 1
    for k, copy in enumerate(copies):
        if k != last:
            copy.start()
    copies[last].start()
    for copy in copies:
        copy.wait()


def local(pair_density, coulomb):
    local_k, bands, width = pair_density.shape
    n_row = lax.axis_size("row")
    m = 2 * n_row * bands
    n = 4 * n_row * bands
    group = n // NX
    rounds = len(PLAN)
    passed = pl.pallas_call(
        kernel,
        out_shape=[
            pltpu.VMEM((NX, m, group), F32),
            pltpu.VMEM((2, len(SHARED), N_TILE, m // 2, 128), F32),
        ],
        in_specs=[pl.BlockSpec(memory_space=pl.ANY), pl.BlockSpec(memory_space=pltpu.VMEM)],
        out_specs=[pl.BlockSpec(memory_space=pltpu.VMEM)] * 2,
        scratch_shapes=[
            pltpu.VMEM((2, 4 * n_row, bands, width), F32),
            pltpu.VMEM((2, NY, 2, n_row, bands, width // NY), F32),
            pltpu.VMEM((2, 8, width), F32),
            pltpu.VMEM((m, 2 * width), BF16),
            pltpu.VMEM((m, 2 * width), BF16),
            pltpu.VMEM((group, 2 * width), BF16),
            pltpu.VMEM((group, 2 * width), BF16),
            pltpu.SemaphoreType.DMA((4 * rounds,)),
            pltpu.SemaphoreType.DMA((4 * rounds,)),
            pltpu.SemaphoreType.DMA((n_row,)),
            pltpu.SemaphoreType.DMA((n_row,)),
            pltpu.SemaphoreType.DMA((64,)),
            pltpu.SemaphoreType.DMA((64,)),
            pltpu.SemaphoreType.DMA((3 * N_TILE,)),
            pltpu.SemaphoreType.DMA((3 * N_TILE,)),
            pltpu.SemaphoreType.DMA((6,)),
        ],
        compiler_params=pltpu.CompilerParams(
            collective_id=0, has_side_effects=True, vmem_limit_bytes=FIRST_LIMIT
        ),
        name="gather_and_contract",
    )(pair_density, coulomb)
    return pl.pallas_call(
        last_kernel,
        out_shape=jax.ShapeDtypeStruct((m, n), F32),
        in_specs=[pl.BlockSpec(memory_space=pltpu.VMEM)] * 2,
        out_specs=pl.BlockSpec(memory_space=pl.ANY),
        scratch_shapes=[
            pltpu.VMEM((1, m, group), F32),
            pltpu.SemaphoreType.DMA((2 * NX,)),
        ],
        compiler_params=pltpu.CompilerParams(vmem_limit_bytes=LAST_LIMIT),
        name="write_result",
    )(*passed)


def solution(mesh):
    placed = (P("row", None, "ga"), P("ga"))
    return jax.shard_map(
        local, mesh=mesh, in_specs=placed, out_specs=P("row", "col"), check_vma=False
    )
```
